32 devices in a mesh: seq: 8 (over z, y), tp: 4 (over x, core).
Axes of the slice: x: 2, y: 2, z: 4, core: 2. Of those that a mesh axis runs over, the one named last changes fastest.
Arguments:
- query: bfloat16 [4096, 8192], P('seq', 'tp'), may hold values from -6 to 6
- key: bfloat16 [4096, 8192], P('seq', 'tp'), may hold values from -6 to 6
- value: bfloat16 [4096, 8192], P('seq', 'tp'), may hold values from -6 to 6
- gain: float32 [8192], P('tp'), may hold values from 0.1 to 1.9
- cotangent: bfloat16 [4096, 8192], P('seq', 'tp'), may hold values from -24 to 24
Outputs:
- normed: bfloat16 [4096, 8192], P('seq', 'tp')
- grad_query: bfloat16 [4096, 8192], P('seq', 'tp')
- grad_key: bfloat16 [4096, 8192], P('seq', 'tp')
- grad_value: bfloat16 [4096, 8192], P('seq', 'tp')
- grad_gain: float32 [8192], P('tp')
The draws below stay inside these ranges and needn't reach their ends.
All inputs are finite; a program needn't handle non-finite values.
Results may differ from the reference program's by a relative error of at most 0.013.
Values may be sent and summed in bfloat16 or wider, within the bound.
A program may use at most 128 MiB of HBM per device.

```python
import jax
import jax.numpy as jnp
from jax import lax

HEADS = 64
HD = 128
TOK_DEV = 512
TOKENS = 4096
WIDTH = 8192
N_SEQ = 8


def draw_cotangent(key, part):
    position = jnp.arange(TOKENS, dtype=jnp.float32)
    scales = 1.0 + 2.0 * position / TOKENS
    noise = jax.random.normal(key, (TOKENS, HEADS * HD), jnp.float32)
    return jnp.clip(noise * scales[:, None], -24.0, 24.0).astype(jnp.bfloat16)


def block_levels(own_key, shape, pieces, low, top_value):
    level, own = 1.0, jax.random.fold_in(own_key, 6)
    for dim, parts in pieces:
        heights = jnp.exp(jax.random.uniform(jax.random.fold_in(own, dim), (parts,), jnp.float32, low / len(pieces), top_value / len(pieces)))
        level = level * jnp.repeat(heights, shape[dim] // parts).reshape([-1 if axis == dim else 1 for axis in range(len(shape))])
    return level


def normal_values(key, dims, deviation, most, cuts=(), held_as=jnp.bfloat16):
    array = jax.random.normal(key, dims, jnp.float32) * deviation
    if len(cuts) > 0:
        array = block_levels(key, dims, cuts, -0.22, 0.18) * array
    return jnp.clip(array, min=-most, max=most).astype(held_as)


def setup_inputs(seed: int = 0) -> dict:
    splits = jax.random.split(jax.random.key(seed), 6)
    return {
        "query": normal_values(splits[0], (TOKENS, WIDTH), 1.0, 6.0, ((0, 8), (1, 4))),
        "key": normal_values(splits[1], (TOKENS, WIDTH), 1.0, 6.0, ((0, 8), (1, 4))),
        "value": normal_values(splits[2], (TOKENS, WIDTH), 1.0, 6.0, ((0, 8), (1, 4))),
        "gain": jnp.clip(1.0 + 0.18 * jax.random.normal(splits[3], (WIDTH,), jnp.float32), 0.1, 1.9),
        "cotangent": draw_cotangent(jax.random.fold_in(splits[5], 71), 0),
    }


epsilon = 1e-06

def reference(query, key, value, gain, cotangent):
    groups = N_SEQ
    full_width = HEADS * HD
    shape_four = (groups, TOK_DEV, HEADS, HD)
    queries = query.reshape(shape_four)
    keys_all = key.reshape(shape_four)
    values_all = value.reshape(shape_four)
    grads_in = cotangent.reshape(groups, TOK_DEV, full_width)
    causal = (jnp.arange(TOK_DEV)[:, None] >= jnp.arange(TOK_DEV)[None, :]).astype(jnp.float32)
    gain_full = gain.astype(jnp.float32)

    def local_state(pair):
        return jnp.einsum('thd,the->hde', pair[0].astype(jnp.float32), pair[1].astype(jnp.float32)).astype(jnp.bfloat16)
    state_low = lax.map(local_state, (keys_all, values_all))
    zero_state = jnp.zeros((1, HEADS, HD, HD), jnp.float32)
    running = jnp.cumsum(state_low.astype(jnp.float32), axis=0)
    prefix_low = jnp.concatenate([zero_state, running[:-1]], 0).astype(jnp.bfloat16)

    def forward_group(items):
        group_query, group_key, group_value, group_grad, group_prefix = items
        query_f = group_query.astype(jnp.float32)
        key_f = group_key.astype(jnp.float32)
        value_f = group_value.astype(jnp.float32)
        prefix_f = group_prefix.astype(jnp.float32)
        scores = (jnp.einsum('thd,shd->hts', query_f, key_f) * causal[None]).astype(jnp.bfloat16)
        attended = jnp.einsum('hts,shd->thd', scores.astype(jnp.float32), value_f) + jnp.einsum('thd,hde->the', query_f, prefix_f)
        attended = attended.reshape(TOK_DEV, full_width)
        inverse = lax.rsqrt(lax.optimization_barrier(jnp.mean(attended * attended, axis=-1)) + epsilon)
        grad_f = group_grad.astype(jnp.float32)
        scaled_grad = grad_f * gain_full
        cross = lax.optimization_barrier(jnp.sum(attended * scaled_grad, axis=-1))
        normed = (attended * inverse[:, None] * gain_full).astype(jnp.bfloat16)
        grad_out = scaled_grad * inverse[:, None] - attended * (inverse ** 3 * cross / full_width)[:, None]
        grad_out = grad_out.astype(jnp.bfloat16).reshape(TOK_DEV, HEADS, HD)
        gain_part = lax.optimization_barrier(jnp.sum(grad_f * attended * inverse[:, None], axis=0))
        grad_f_out = grad_out.astype(jnp.float32)
        back_scores = (jnp.einsum('thd,shd->hts', grad_f_out, value_f) * causal[None]).astype(jnp.bfloat16)
        grad_q = jnp.einsum('hts,shd->thd', back_scores.astype(jnp.float32), key_f) + jnp.einsum('the,hde->thd', grad_f_out, prefix_f)
        block_grad = jnp.einsum('thd,the->hde', query_f, grad_f_out).astype(jnp.bfloat16)
        return (normed, grad_q.astype(jnp.bfloat16), grad_out, block_grad, gain_part)
    normed, grad_q, grad_outs, grad_low, gain_parts = lax.map(forward_group, (queries, keys_all, values_all, grads_in, prefix_low))
    running_back = jnp.cumsum(grad_low.astype(jnp.float32)[::-1], axis=0)[::-1]
    suffix_low = jnp.concatenate([running_back[1:], zero_state], 0).astype(jnp.bfloat16)

    def backward_group(items):
        group_query, group_key, group_value, group_out, group_suffix = items
        query_f = group_query.astype(jnp.float32)
        key_f = group_key.astype(jnp.float32)
        value_f = group_value.astype(jnp.float32)
        out_f = group_out.astype(jnp.float32)
        suffix_f = group_suffix.astype(jnp.float32)
        scores = (jnp.einsum('thd,shd->hts', query_f, key_f) * causal[None]).astype(jnp.bfloat16)
        back_scores = (jnp.einsum('thd,shd->hts', out_f, value_f) * causal[None]).astype(jnp.bfloat16)
        grad_k = jnp.einsum('hts,thd->shd', back_scores.astype(jnp.float32), query_f) + jnp.einsum('she,hde->shd', value_f, suffix_f)
        grad_v = jnp.einsum('hts,the->she', scores.astype(jnp.float32), out_f) + jnp.einsum('shd,hde->she', key_f, suffix_f)
        return (grad_k.astype(jnp.bfloat16), grad_v.astype(jnp.bfloat16))
    grad_k, grad_v = lax.map(backward_group, (queries, keys_all, values_all, grad_outs, suffix_low))
    flat = (TOKENS, full_width)
    return (normed.reshape(flat), grad_q.reshape(flat), grad_k.reshape(flat), grad_v.reshape(flat), lax.optimization_barrier(jnp.sum(gain_parts, axis=0)))
```

```python
import functools

import jax
import jax.numpy as jnp
from jax import lax
from jax.experimental import pallas as pl
from jax.experimental.pallas import tpu as pltpu
from jax.sharding import PartitionSpec as P

HD = 128
epsilon = 1e-06
MESH = pl.DeviceIdType.MESH
F32 = jnp.float32
BF16 = jnp.bfloat16


def dot(a, b, ca, cb):
    return lax.dot_general(a, b, (((ca,), (cb,)), ((), ())), preferred_element_type=F32)


def kernel(
    n, ntp, inner, group, full_width,
    q_hbm, k_hbm, v_hbm, gain_ref, cot_hbm,
    normed_hbm, gq_hbm, gk_hbm, gv_hbm, gg_out,
    qb, kb, vb, cb, attb, goutb, gkb, gvb, nst, qst, kst, vst,
    fy, fzin, fzout, flow, by, bzin, bzout, blow,
    acc_sq, acc_cr, inv_b, coef_b, tpb, ggb,
    in_sem, out_sem,
    fys, fyr, fzs, fzr, bys, byr, bzs, bzr, tps, tpr, ggs, ggr,
):
    rows, width = qb.shape
    heads = width // HD
    chunks = heads // group
    outer = n // inner
    block = min(rows, 256)
    nblocks = rows // block
    me = lax.axis_index("seq")
    mt = lax.axis_index("tp")
    z = me // inner
    y = me % inner
    cw = group * HD

    def ccols(c):
        return pl.ds(pl.multiple_of(c * cw, cw), cw)

    def hcols(h):
        return pl.ds(pl.multiple_of(h * HD, HD), HD)

    ins = ((k_hbm, kb), (v_hbm, vb), (q_hbm, qb), (cot_hbm, cb))
    outs = ((nst, normed_hbm), (qst, gq_hbm), (kst, gk_hbm), (vst, gv_hbm))

    def in_copy(i, c):
        src, dst = ins[i]
        return pltpu.make_async_copy(src.at[:, ccols(c)], dst.at[:, ccols(c)], in_sem.at[i, c])

    def out_copy(i, c):
        src, dst = outs[i]
        return pltpu.make_async_copy(src.at[:, ccols(c)], dst.at[:, ccols(c)], out_sem.at[i, c])

    def loop(count, body):
        def step(i, carry):
            body(i)
            return carry
        lax.fori_loop(0, count, step, 0)

    def start_kv(c):
        in_copy(0, c).start()
        in_copy(1, c).start()

    def start_qc(c):
        in_copy(2, c).start()
        in_copy(3, c).start()

    loop(chunks, start_kv)
    loop(chunks, start_qc)

    barrier = pltpu.get_barrier_semaphore()

    def greet_seq(r):
        pl.semaphore_signal(barrier, inc=1, device_id={"seq": (me + 1 + r) % n}, device_id_type=MESH)

    def greet_tp(r):
        pl.semaphore_signal(barrier, inc=1, device_id={"tp": (mt + 1 + r) % ntp}, device_id_type=MESH)

    loop(n - 1, greet_seq)
    loop(ntp - 1, greet_tp)
    pl.semaphore_wait(barrier, n - 1 + ntp - 1)

    def row_send(c, r, buf, ssem, rsem):
        peer = (y + r) % inner
        return pltpu.make_async_remote_copy(
            src_ref=buf.at[y, c], dst_ref=buf.at[y, c],
            send_sem=ssem.at[peer, c], recv_sem=rsem.at[y, c],
            device_id={"seq": z * inner + peer}, device_id_type=MESH)

    def row_recv(c, r, buf, ssem, rsem):
        peer = (y + r) % inner
        return pltpu.make_async_remote_copy(
            src_ref=buf.at[peer, c], dst_ref=buf.at[peer, c],
            send_sem=ssem.at[peer, c], recv_sem=rsem.at[peer, c],
            device_id={"seq": z * inner + peer}, device_id_type=MESH)

    def chain(c, step, zin, zout, zs, zr):
        target = (me + step * inner + n) % n
        return pltpu.make_async_remote_copy(
            src_ref=zout.at[c], dst_ref=zin.at[c],
            send_sem=zs.at[c], recv_sem=zr.at[c],
            device_id={"seq": target}, device_id_type=MESH)

    def relay(c, step, buf, ys, yr, zin, zout, zs, zr, low, first, last):
        for r in range(1, inner):
            row_recv(c, r, buf, ys, yr).wait_recv()

        @pl.when(first)
        def _():
            zin[c] = jnp.zeros(zin.shape[1:], BF16)

        @pl.when(jnp.logical_not(first))
        def _():
            chain(c, step, zin, zout, zs, zr).wait_recv()

        @pl.when(jnp.logical_not(last))
        def _():
            total = zin[c].astype(F32)
            for other in range(inner):
                total = total + buf[other, c].astype(F32)
            zout[c] = total.astype(BF16)
            chain(c, step, zin, zout, zs, zr).start()

        mine = zin[c].astype(F32)
        for other in range(inner):
            before = (other < y) if step > 0 else (other > y)
            mine = mine + buf[other, c].astype(F32) * before.astype(F32)
        low[c] = mine.astype(BF16)

    def forward_state(c):
        in_copy(0, c).wait()
        in_copy(1, c).wait()
        for g in range(group):
            cols = hcols(c * group + g)
            fy[y, c, g] = dot(kb[:, cols], vb[:, cols], 0, 0).astype(BF16)
        for r in range(1, inner):
            row_send(c, r, fy, fys, fyr).start()

    loop(chunks, forward_state)
    acc_sq[...] = jnp.zeros_like(acc_sq)
    acc_cr[...] = jnp.zeros_like(acc_cr)

    def below(first_row, first_col, shape, transposed):
        row = first_row + lax.broadcasted_iota(jnp.int32, shape, 0)
        col = first_col + lax.broadcasted_iota(jnp.int32, shape, 1)
        return (row <= col) if transposed else (row >= col)

    def forward_local(c):
        in_copy(2, c).wait()
        in_copy(3, c).wait()
        for g in range(group):
            cols = hcols(c * group + g)
            for i in range(nblocks):
                mine = pl.ds(i * block, block)
                seen = pl.ds(0, (i + 1) * block)
                s = dot(qb[mine, cols], kb[seen, cols], 1, 1)
                s = jnp.where(below(i * block, 0, s.shape, False), s, 0.0).astype(BF16)
                attb[mine, cols] = dot(s, vb[seen, cols], 1, 0)

    def forward_finish(c):
        for g in range(group):
            cols = hcols(c * group + g)
            att = attb[:, cols] + dot(qb[:, cols], flow[c, g], 1, 0)
            attb[:, cols] = att
            scaled = cb[:, cols].astype(F32) * gain_ref[:, cols]
            acc_sq[...] += att * att
            acc_cr[...] += att * scaled

    first_z = z == 0
    last_z = z == outer - 1
    f_skew = jnp.minimum(1 + 2 * z, chunks)

    def forward_slot(s):
        @pl.when(s < chunks)
        def _():
            forward_local(s)

        c = s - f_skew

        @pl.when(jnp.logical_and(c >= 0, c < chunks))
        def _():
            relay(c, 1, fy, fys, fyr, fzin, fzout, fzs, fzr, flow, first_z, last_z)
            forward_finish(c)

    loop(chunks + f_skew, forward_slot)

    upper = lax.broadcasted_iota(jnp.int32, (8, HD), 0) < 4
    pick_sq = upper.astype(F32)
    pick_cr = 1.0 - pick_sq

    def rowsum(pick, acc):
        return lax.dot_general(
            pick, acc[...], (((1,), (1,)), ((), ())),
            precision=lax.Precision.HIGHEST, preferred_element_type=F32)

    tpb[mt] = rowsum(pick_sq, acc_sq) + rowsum(pick_cr, acc_cr)

    def tp_send(r):
        peer = (mt + r) % ntp
        return pltpu.make_async_remote_copy(
            src_ref=tpb.at[mt], dst_ref=tpb.at[mt], send_sem=tps.at[peer], recv_sem=tpr.at[mt],
            device_id={"tp": peer}, device_id_type=MESH)

    def tp_recv(r):
        peer = (mt + r) % ntp
        return pltpu.make_async_remote_copy(
            src_ref=tpb.at[peer], dst_ref=tpb.at[peer], send_sem=tps.at[peer], recv_sem=tpr.at[peer],
            device_id={"tp": peer}, device_id_type=MESH)

    for r in range(1, ntp):
        tp_send(r).start()
    for r in range(1, ntp):
        tp_recv(r).wait_recv()
    total = tpb[0]
    for i in range(1, ntp):
        total = total + tpb[i]
    inv_row = lax.rsqrt(total[0:1, :] / full_width + epsilon)
    coef_row = inv_row * inv_row * inv_row * total[4:5, :] / full_width
    half = lax.broadcasted_iota(jnp.int32, (8, rows), 0) < 4
    both = jnp.transpose(jnp.where(half, inv_row, coef_row))
    inv_b[...] = jnp.broadcast_to(both[:, 0:1], (rows, HD))
    coef_b[...] = jnp.broadcast_to(both[:, 4:5], (rows, HD))

    def backward_state(c):
        for g in range(group):
            h = c * group + g
            cols = hcols(h)
            inv = inv_b[...]
            gain = gain_ref[:, cols]
            att = attb[:, cols]
            grad = cb[:, cols].astype(F32)
            gout = (grad * gain * inv - att * coef_b[...]).astype(BF16)
            goutb[:, cols] = gout
            by[y, c, g] = dot(qb[:, cols], gout, 0, 0).astype(BF16)
            unit = att * inv
            nst[:, cols] = (unit * gain).astype(BF16)
            ggb[me, pl.ds(h, 1), :] = jnp.sum(grad * unit, axis=0, keepdims=True)
        for r in range(1, inner):
            row_send(c, r, by, bys, byr).start()
        out_copy(0, c).start()

    loop(chunks, backward_state)

    def gg_send(peer):
        return pltpu.make_async_remote_copy(
            src_ref=ggb.at[me], dst_ref=ggb.at[me], send_sem=ggs.at[peer], recv_sem=ggr.at[me],
            device_id={"seq": peer}, device_id_type=MESH)

    def gg_recv(peer):
        return pltpu.make_async_remote_copy(
            src_ref=ggb.at[peer], dst_ref=ggb.at[peer], send_sem=ggs.at[peer], recv_sem=ggr.at[peer],
            device_id={"seq": peer}, device_id_type=MESH)

    loop(n - 1, lambda r: gg_send((me + 1 + r) % n).start())

    def backward_local(c):
        for g in range(group):
            cols = hcols(c * group + g)
            for i in range(nblocks):
                mine = pl.ds(i * block, block)
                seen = pl.ds(0, (i + 1) * block)
                later = pl.ds(i * block, rows - i * block)
                go = goutb[mine, cols]
                b = dot(go, vb[seen, cols], 1, 1)
                b = jnp.where(below(i * block, 0, b.shape, False), b, 0.0).astype(BF16)
                gq = dot(b, kb[seen, cols], 1, 0) + dot(go, flow[c, g], 1, 1)
                qst[mine, cols] = gq.astype(BF16)
                bt = dot(vb[mine, cols], goutb[later, cols], 1, 1)
                keep = below(0, 0, bt.shape, True)
                bt = jnp.where(keep, bt, 0.0).astype(BF16)
                gkb[mine, cols] = dot(bt, qb[later, cols], 1, 0)
                st = dot(kb[mine, cols], qb[later, cols], 1, 1)
                st = jnp.where(keep, st, 0.0).astype(BF16)
                gvb[mine, cols] = dot(st, goutb[later, cols], 1, 0)
        out_copy(1, c).start()

    def backward_finish(c):
        for g in range(group):
            cols = hcols(c * group + g)
            suffix = blow[c, g]
            kst[:, cols] = (gkb[:, cols] + dot(vb[:, cols], suffix, 1, 1)).astype(BF16)
            vst[:, cols] = (gvb[:, cols] + dot(kb[:, cols], suffix, 1, 0)).astype(BF16)
        out_copy(2, c).start()
        out_copy(3, c).start()

    b_skew = jnp.minimum(1 + 2 * (outer - 1 - z), chunks)

    def backward_slot(s):
        @pl.when(s < chunks)
        def _():
            backward_local(s)

        c = s - b_skew

        @pl.when(jnp.logical_and(c >= 0, c < chunks))
        def _():
            relay(c, -1, by, bys, byr, bzin, bzout, bzs, bzr, blow, last_z, first_z)
            backward_finish(c)

    loop(chunks + b_skew, backward_slot)

    loop(n - 1, lambda r: gg_recv((me + 1 + r) % n).wait_recv())
    gain_total = ggb[0]
    for i in range(1, n):
        gain_total = gain_total + ggb[i]
    gg_out[...] = gain_total

    loop(n - 1, lambda r: gg_send((me + 1 + r) % n).wait_send())
    for r in range(1, ntp):
        tp_send(r).wait_send()

    def drain(c):
        for r in range(1, inner):
            row_send(c, r, fy, fys, fyr).wait_send()
            row_send(c, r, by, bys, byr).wait_send()

        @pl.when(jnp.logical_not(last_z))
        def _():
            chain(c, 1, fzin, fzout, fzs, fzr).wait_send()

        @pl.when(jnp.logical_not(first_z))
        def _():
            chain(c, -1, bzin, bzout, bzs, bzr).wait_send()

        for i in range(4):
            out_copy(i, c).wait()

    loop(chunks, drain)


def local(n, ntp, query, key, value, gain, cotangent):
    rows, width = query.shape
    heads = width // HD
    group = 2 if heads % 2 == 0 else 1
    chunks = heads // group
    inner = 1
    while n % (inner * inner * 4) == 0:
        inner *= 2
    state = (chunks, group, HD, HD)
    wide = lambda t: pltpu.VMEM((rows, width), t)
    states = lambda: [
        pltpu.VMEM((inner, *state), BF16), pltpu.VMEM(state, BF16),
        pltpu.VMEM(state, BF16), pltpu.VMEM(state, BF16)]
    dma = pltpu.SemaphoreType.DMA
    sems = lambda: [dma((inner, chunks)), dma((inner, chunks)), dma((chunks,)), dma((chunks,))]
    any_spec = pl.BlockSpec(memory_space=pl.ANY)
    vmem_spec = pl.BlockSpec(memory_space=pltpu.VMEM)
    big = jax.ShapeDtypeStruct((rows, width), BF16)
    outs = pl.pallas_call(
        functools.partial(kernel, n, ntp, inner, group, ntp * width),
        out_shape=[big, big, big, big, jax.ShapeDtypeStruct((heads, HD), F32)],
        in_specs=[any_spec, any_spec, any_spec, vmem_spec, any_spec],
        out_specs=[any_spec, any_spec, any_spec, any_spec, vmem_spec],
        scratch_shapes=[
            wide(BF16), wide(BF16), wide(BF16), wide(BF16),
            wide(F32), wide(BF16), wide(F32), wide(F32),
            wide(BF16), wide(BF16), wide(BF16), wide(BF16),
            *states(), *states(),
            pltpu.VMEM((rows, HD), F32), pltpu.VMEM((rows, HD), F32),
            pltpu.VMEM((rows, HD), F32), pltpu.VMEM((rows, HD), F32),
            pltpu.VMEM((ntp, 8, rows), F32), pltpu.VMEM((n, heads, HD), F32),
            dma((4, chunks)), dma((4, chunks)),
            *sems(), *sems(),
            dma((ntp,)), dma((ntp,)), dma((n,)), dma((n,)),
        ],
        compiler_params=pltpu.CompilerParams(
            collective_id=0, has_side_effects=True, vmem_limit_bytes=60 * 1024 * 1024),
    )(query, key, value, gain.reshape(1, width), cotangent)
    return (*outs[:4], outs[4].reshape(width))


def solution(mesh):
    return jax.shard_map(
        functools.partial(local, mesh.shape["seq"], mesh.shape["tp"]),
        mesh=mesh,
        in_specs=(P("seq", "tp"), P("seq", "tp"), P("seq", "tp"), P("tp"), P("seq", "tp")),
        out_specs=(P("seq", "tp"), P("seq", "tp"), P("seq", "tp"), P("seq", "tp"), P("tp")),
        check_vma=False,
    )
```
